8 devices in a mesh: row: 4 (over z, y, x), col: 2 (over core).
Axes of the slice: x: 2, y: 2, z: 1, core: 2. Of those that a mesh axis runs over, the one named last changes fastest.
Arguments:
- v_mat: float32 [8192, 8192], P('row', 'col')
- t_fac: float32 [128, 64, 64], P('col')
- z_vec: float32 [8192, 2048], P(None, ('col', 'row'))
Outputs:
- output: float32 [8192, 2048], P('row', 'col')
All inputs are finite; a program needn't handle non-finite values.
Results may differ from the reference program's by a relative error of at most 0.001.
Values sent between devices are 32-bit elements.
A program may use at most 1 GiB of HBM per device.

```python
import jax
import jax.numpy as jnp
from jax import lax

MAT_ORDER = 8192
PANEL_WIDTH = 64
NUM_VECTORS = 2048
ROW_SHARDS = 4
COL_SHARDS = 2


def stored_to_global(mat_order, panel_width, shards):
    stored_idx = jnp.arange(mat_order, dtype=jnp.int32)
    per_shard = mat_order // shards
    shard_idx = stored_idx // per_shard
    within = stored_idx % per_shard
    block_idx = within // panel_width
    offset = within % panel_width
    return (block_idx * shards + shard_idx) * panel_width + offset


def build_factors(v_mat):
    panels = v_mat.reshape(MAT_ORDER, MAT_ORDER // PANEL_WIDTH, PANEL_WIDTH)
    gram_mat = jnp.einsum('nsb,nse->sbe', panels, panels)
    half_diag = 0.5 * jnp.diagonal(gram_mat, axis1=1, axis2=2)
    inv_factor = jnp.triu(gram_mat, 1) + half_diag[:, :, None] * jnp.eye(PANEL_WIDTH, dtype=jnp.float32)
    return jnp.triu(jnp.linalg.inv(inv_factor))


def setup_inputs(seed: int = 0) -> dict:
    rng_key = jax.random.key(seed)
    key_v, key_z = jax.random.split(rng_key)
    raw_vals = jax.random.normal(key_v, (MAT_ORDER, MAT_ORDER), jnp.float32)
    row_ids = stored_to_global(MAT_ORDER, PANEL_WIDTH, ROW_SHARDS)[:, None]
    col_ids = stored_to_global(MAT_ORDER, PANEL_WIDTH, COL_SHARDS)[None, :]
    unit_diag = (row_ids == col_ids).astype(jnp.float32)
    v_mat = jnp.where(row_ids > col_ids, raw_vals, unit_diag)
    t_fac = build_factors(v_mat)
    z_vec = jax.random.normal(key_z, (MAT_ORDER, NUM_VECTORS), jnp.float32)
    return {'v_mat': v_mat, 't_fac': t_fac, 'z_vec': z_vec}


def reference(v_mat, t_fac, z_vec):
    num_panels = MAT_ORDER // PANEL_WIDTH
    local_panels = num_panels // COL_SHARDS

    def apply_panel(x_cur, panel_idx):
        panel_slot = (panel_idx % COL_SHARDS) * local_panels + panel_idx // COL_SHARDS
        v_pan = lax.dynamic_slice_in_dim(v_mat, panel_slot * PANEL_WIDTH, PANEL_WIDTH, axis=1)
        t_pan = lax.dynamic_index_in_dim(t_fac, panel_slot, axis=0, keepdims=False)
        w_blk = jnp.dot(v_pan.T, x_cur, preferred_element_type=jnp.float32)
        y_blk = jnp.dot(t_pan, w_blk, preferred_element_type=jnp.float32)
        x_new = x_cur - jnp.dot(v_pan, y_blk, preferred_element_type=jnp.float32)
        return x_new, None

    x_out, _ = lax.scan(apply_panel, z_vec, jnp.arange(num_panels - 1, -1, -1))
    return x_out
```

```python
import functools

import jax
import jax.numpy as jnp
from jax import lax
from jax.experimental import pallas as pl
from jax.experimental.pallas import tpu as pltpu
from jax.sharding import PartitionSpec as P

MESH = pl.DeviceIdType.MESH
HIGHEST = lax.Precision.HIGHEST
F32, BF16 = jnp.float32, jnp.bfloat16

STEPS = 32
TILE = 256
LOC_ROWS = 2048
OWN_AHEAD = 6
FWD_AHEAD = 3
DIAG_AHEAD = 1

NN = (((1,), (0,)), ((), ()))
NT = (((1,), (1,)), ((), ()))
TN = (((0,), (0,)), ((), ()))


def dot32(a, b, dims=NN):
    return lax.dot_general(a, b, dims, precision=HIGHEST, preferred_element_type=F32)


def dotb(a, b, dims=NN):
    return lax.dot_general(a, b, dims, preferred_element_type=F32)


def split3(x):
    hi = x.astype(BF16)
    rest = x - hi.astype(F32)
    mid = rest.astype(BF16)
    low = (rest - mid.astype(F32)).astype(BF16)
    return hi, mid, low


def six(a, b, dims):
    ah, am, al = a
    bh, bm, bl = b
    return (dotb(ah, bh, dims) + dotb(ah, bm, dims) + dotb(am, bh, dims)
            + dotb(am, bm, dims) + dotb(ah, bl, dims) + dotb(al, bh, dims))


X_DIR, Y_DIR, Y_FWD, X_FWD, S_OWN, S_X, S_Y, S_DA, S_DB = range(9)


def kernel(v_ref, t_ref, z_ref, out_ref, g_ref,
           xt, vbuf, vs, stage, t_own, t_sib, dmat, wt, gm, yt,
           send_sem, recv_sem, load_sem, aux_sem, fin_send, fin_recv,
           *, comm=True, compute=True):
    r = lax.axis_index("row")
    c = lax.axis_index("col")
    rx = r + 1 - 2 * lax.rem(r, 2)
    ry = lax.rem(r + 2, 4)
    rd = 3 - r
    dev_x, dev_y, dev_d, dev_s = (rx, c), (ry, c), (rd, c), (r, 1 - c)
    peer_row = (r, rx, ry, rd)

    barrier = pltpu.get_barrier_semaphore()
    for dev in (dev_x, dev_y, dev_d, dev_s):
        pl.semaphore_signal(barrier, inc=1, device_id=dev, device_id_type=MESH)
    pl.semaphore_wait(barrier, 4)

    def win(n, part=None):
        m = STEPS - 1 - n
        lo, rows = 64 * m, 64 * (n + 1)
        if part == 0:
            rows = rows // 2
        elif part == 1:
            lo, rows = lo + rows // 2, rows // 2
        return pl.ds(lo, rows), pl.ds(128 * m, 128)

    def mk(cls, n):
        part = {Y_FWD: 0, S_DA: 0, X_FWD: 1, S_DB: 1}.get(cls)
        a, b = win(n, part)
        own = v_ref.at[a, b]
        if cls == X_DIR:
            src, dst, dev = own, g_ref.at[1, 0, a, b], dev_x
        elif cls == Y_DIR:
            src, dst, dev = own, g_ref.at[2, 0, a, b], dev_y
        elif cls == Y_FWD:
            src, dst, dev = g_ref.at[1, 0, a, b], g_ref.at[3, 0, a, b], dev_y
        elif cls == X_FWD:
            src, dst, dev = g_ref.at[2, 0, a, b], g_ref.at[3, 0, a, b], dev_x
        elif cls == S_OWN:
            src, dst, dev = own, g_ref.at[0, 1, a, b], dev_s
        elif cls == S_X:
            src, dst, dev = g_ref.at[1, 0, a, b], g_ref.at[1, 1, a, b], dev_s
        elif cls == S_Y:
            src, dst, dev = g_ref.at[2, 0, a, b], g_ref.at[2, 1, a, b], dev_s
        else:
            src, dst, dev = g_ref.at[3, 0, a, b], g_ref.at[3, 1, a, b], dev_s
        return pltpu.make_async_remote_copy(
            src_ref=src, dst_ref=dst, send_sem=send_sem.at[cls, n],
            recv_sem=recv_sem.at[cls, n], device_id=dev, device_id_type=MESH)

    def own_send(n):
        for cls in (X_DIR, Y_DIR, S_OWN):
            mk(cls, n).start()

    def forward(n):
        mk(X_DIR, n).wait_recv()
        mk(Y_FWD, n).start()
        mk(S_X, n).start()
        mk(Y_DIR, n).wait_recv()
        mk(X_FWD, n).start()
        mk(S_Y, n).start()

    def share_diag(n):
        mk(Y_FWD, n).wait_recv()
        mk(S_DA, n).start()
        mk(X_FWD, n).wait_recv()
        mk(S_DB, n).start()

    def sib_wait(n):
        for cls in (S_OWN, S_X, S_Y, S_DA, S_DB):
            mk(cls, n).wait_recv()

    def vloads(n):
        a, b = win(n)
        cps = []
        for k in range(4):
            for cc in range(2):
                src = v_ref.at[a, b] if (k == 0 and cc == 0) else g_ref.at[k, cc, a, b]
                cps.append(pltpu.make_async_copy(
                    src, vbuf.at[k, a, pl.ds(128 * cc, 128)], load_sem.at[2 * k + cc]))
        return cps

    fwd_at = {n: [] for n in range(-1, STEPS)}
    diag_at = {n: [] for n in range(-1, STEPS)}
    for n in range(STEPS):
        fwd_at[max(n - FWD_AHEAD, -1) if n < STEPS - 1 else n - 2].append(n)
        diag_at[max(n - DIAG_AHEAD, -1) if n < STEPS - 1 else n].append(n)

    t_local = pltpu.make_async_copy(t_ref, t_own, aux_sem.at[0])
    t_local.start()
    t_remote = pltpu.make_async_remote_copy(
        src_ref=t_ref, dst_ref=t_sib, send_sem=aux_sem.at[1], recv_sem=aux_sem.at[2],
        device_id=dev_s, device_id_type=MESH)
    t_remote.start()
    zl = [pltpu.make_async_copy(
        z_ref.at[pl.ds(pl.multiple_of(peer_row[k] * LOC_ROWS, LOC_ROWS), LOC_ROWS), :],
        stage.at[k], aux_sem.at[3 + k]) for k in range(4)]
    for cp in zl:
        cp.start()
    if comm:
        for n in range(OWN_AHEAD):
            own_send(n)

    vbuf[...] = jnp.zeros_like(vbuf)
    dmat[...] = jnp.zeros_like(dmat)
    for cp in zl:
        cp.wait()

    @pl.loop(0, 32)
    def _(t):
        k, i4 = lax.rem(t, 4), t // 4
        xt[t] = stage[k, pl.ds(pl.multiple_of(i4 * TILE, TILE), TILE), :].T

    t_local.wait()
    t_remote.wait()
    if comm:
        for n in fwd_at[-1]:
            forward(n)
        for n in diag_at[-1]:
            share_diag(n)

    def order(dim):
        pos = lax.broadcasted_iota(jnp.int32, (TILE, TILE), dim) // 64
        core = pos // 2
        return 2 * (pos - 2 * core) + core + c - 2 * core * c

    def block(n):
        m = STEPS - 1 - n
        first = 4 * (m // 4)
        for i in range(2):
            dmat[64 * i:64 * i + 64, 64 * i:64 * i + 64] = t_own[2 * m + i]
            dmat[128 + 64 * i:192 + 64 * i, 128 + 64 * i:192 + 64 * i] = t_sib[2 * m + i]
        wt[...] = jnp.zeros_like(wt)
        gm[...] = jnp.zeros_like(gm)

        @pl.loop(first, 32)
        def _(t):
            k, i4 = lax.rem(t, 4), t // 4
            v = split3(vbuf[k, pl.ds(pl.multiple_of(i4 * TILE, TILE), TILE), :])
            for i in range(3):
                vs[i, t] = v[i]
            x = split3(xt[t])
            wt[...] += six(x, v, NN)
            gm[0] += dotb(v[0], v[0], TN) + dotb(v[1], v[1], TN)
            gm[1] += dotb(v[0], v[1], TN) + dotb(v[0], v[2], TN)

        cross = gm[1]
        gram = gm[0] + cross + cross.T
        upper = jnp.where(order(0) < order(1), gram, 0.0)
        diag = dmat[...]
        nil = dot32(diag, upper)
        sq = dot32(nil, nil)
        eye = (lax.broadcasted_iota(jnp.int32, (TILE, TILE), 0)
               == lax.broadcasted_iota(jnp.int32, (TILE, TILE), 1)).astype(F32)
        big = dot32(dot32(eye - nil, eye + sq), diag)
        y = split3(dot32(wt[...], big, NT))
        for i in range(3):
            yt[i] = y[i]

        @pl.loop(first, 32)
        def _(t):
            xt[t] -= six((yt[0], yt[1], yt[2]), (vs[0, t], vs[1, t], vs[2, t]), NT)

    @pl.loop(0, STEPS)
    def _(n):
        for k in range(STEPS):
            @pl.when(n == k)
            def _(k=k):
                if comm:
                    if k + OWN_AHEAD < STEPS:
                        own_send(k + OWN_AHEAD)
                    for j in fwd_at[k]:
                        forward(j)
                    for j in diag_at[k]:
                        share_diag(j)
                    sib_wait(k)
                loads = vloads(k)
                for cp in loads:
                    cp.start()
                for cp in loads:
                    cp.wait()
        if compute:
            block(n)

    finals = {}
    for k in (3, 1, 2, 0):
        @pl.loop(0, 8)
        def _(i4, k=k):
            stage[k, pl.ds(pl.multiple_of(i4 * TILE, TILE), TILE), :] = xt[4 * i4 + k].T
        cols = out_ref.at[:, pl.ds(pl.multiple_of(r * TILE, TILE), TILE)]
        if k:
            finals[k] = pltpu.make_async_remote_copy(
                src_ref=stage.at[k], dst_ref=cols, send_sem=fin_send.at[k],
                recv_sem=fin_recv.at[k], device_id=(peer_row[k], c), device_id_type=MESH)
        else:
            finals[k] = pltpu.make_async_copy(stage.at[0], cols, fin_send.at[0])
        finals[k].start()
    if comm:
        for n in range(STEPS):
            for cls in range(9):
                mk(cls, n).wait_send()
    for k in range(4):
        finals[k].wait()


def solution(mesh, comm=True, compute=True):
    def local_body(v_loc, t_loc, z_loc):
        any_spec = pl.BlockSpec(memory_space=pl.ANY)
        out, _ = pl.pallas_call(
            functools.partial(kernel, comm=comm, compute=compute),
            out_shape=(jax.ShapeDtypeStruct((LOC_ROWS, 4 * TILE), F32),
                       jax.ShapeDtypeStruct((4, 2, LOC_ROWS, 4096), F32)),
            in_specs=[any_spec] * 3,
            out_specs=(any_spec, any_spec),
            scratch_shapes=[
                pltpu.VMEM((32, TILE, TILE), F32),
                pltpu.VMEM((4, LOC_ROWS, TILE), F32),
                pltpu.VMEM((3, 32, TILE, TILE), BF16),
                pltpu.VMEM((4, LOC_ROWS, TILE), F32),
                pltpu.VMEM((64, 64, 64), F32),
                pltpu.VMEM((64, 64, 64), F32),
                pltpu.VMEM((TILE, TILE), F32),
                pltpu.VMEM((TILE, TILE), F32),
                pltpu.VMEM((2, TILE, TILE), F32),
                pltpu.VMEM((3, TILE, TILE), BF16),
                pltpu.SemaphoreType.DMA((9, STEPS)),
                pltpu.SemaphoreType.DMA((9, STEPS)),
                pltpu.SemaphoreType.DMA((8,)),
                pltpu.SemaphoreType.DMA((7,)),
                pltpu.SemaphoreType.DMA((4,)),
                pltpu.SemaphoreType.DMA((4,)),
            ],
            compiler_params=pltpu.CompilerParams(
                collective_id=0, has_side_effects=True, vmem_limit_bytes=60 * 2**20),
            name="apply_panels",
        )(v_loc, t_loc, z_loc)
        return out

    return jax.shard_map(local_body, mesh=mesh,
                         in_specs=(P('row', 'col'), P('col', None, None), P(None, ('col', 'row'))),
                         out_specs=P('row', 'col'), check_vma=False)
```

```python
import functools

import jax
import jax.numpy as jnp
from jax import lax
from jax.experimental import pallas as pl
from jax.experimental.pallas import tpu as pltpu
from jax.sharding import PartitionSpec as P

MESH = pl.DeviceIdType.MESH
HIGHEST = lax.Precision.HIGHEST
F32, BF16 = jnp.float32, jnp.bfloat16

STEPS = 32
TILE = 256
LOC_ROWS = 2048


def ahead(n, early, late):
    return early if n < 14 else max(late, early - (n - 14))


def plan(early, late):
    at = {k: [] for k in range(-1, STEPS)}
    for n in range(STEPS):
        at[max(n - ahead(n, early, late), -1)].append(n)
    return at


OWN_AT = plan(8, 4)
FWD_AT = plan(4, 3)
DIAG_AT = plan(2, 1)

NN = (((1,), (0,)), ((), ()))
NT = (((1,), (1,)), ((), ()))
TN = (((0,), (0,)), ((), ()))


def dot32(a, b, dims=NN):
    return lax.dot_general(a, b, dims, precision=HIGHEST, preferred_element_type=F32)


def dotb(a, b, dims=NN):
    return lax.dot_general(a, b, dims, preferred_element_type=F32)


def split3(x):
    hi = x.astype(BF16)
    rest = x - hi.astype(F32)
    mid = rest.astype(BF16)
    low = (rest - mid.astype(F32)).astype(BF16)
    return hi, mid, low


def six(a, b, dims):
    (ldim,), (rdim,) = dims[0]
    lhs = [x[i] for x in a for i in (0, 0, 1, 1, 0, 2)]
    rhs = [x[i] for x in b for i in (0, 1, 0, 1, 2, 0)]
    return dotb(jnp.concatenate(lhs, axis=ldim), jnp.concatenate(rhs, axis=rdim), dims)


X_DIR, Y_DIR, Y_FWD, X_FWD, S_OWN, S_X, S_Y, S_DA, S_DB = range(9)


def kernel(v_ref, t_ref, z_ref, out_ref, g_ref,
           xt, vbuf, vs, stage, t_own, t_sib, dmat, wt, gm, yt,
           send_sem, recv_sem, load_sem, aux_sem, fin_send, fin_recv,
           *, comm=True, compute=True):
    r = lax.axis_index("row")
    c = lax.axis_index("col")
    rx = r + 1 - 2 * lax.rem(r, 2)
    ry = lax.rem(r + 2, 4)
    rd = 3 - r
    dev_x, dev_y, dev_d, dev_s = (rx, c), (ry, c), (rd, c), (r, 1 - c)
    peer_row = (r, rx, ry, rd)

    barrier = pltpu.get_barrier_semaphore()
    for dev in (dev_x, dev_y, dev_d, dev_s):
        pl.semaphore_signal(barrier, inc=1, device_id=dev, device_id_type=MESH)
    pl.semaphore_wait(barrier, 4)

    def win(n, part=None):
        m = STEPS - 1 - n
        lo, rows = 64 * m, 64 * (n + 1)
        if part == 0:
            rows = rows // 2
        elif part == 1:
            lo, rows = lo + rows // 2, rows // 2
        return pl.ds(lo, rows), pl.ds(128 * m, 128)

    def mk(cls, n):
        part = {Y_FWD: 0, S_DA: 0, X_FWD: 1, S_DB: 1}.get(cls)
        a, b = win(n, part)
        own = v_ref.at[a, b]
        if cls == X_DIR:
            src, dst, dev = own, g_ref.at[1, 0, a, b], dev_x
        elif cls == Y_DIR:
            src, dst, dev = own, g_ref.at[2, 0, a, b], dev_y
        elif cls == Y_FWD:
            src, dst, dev = g_ref.at[1, 0, a, b], g_ref.at[3, 0, a, b], dev_y
        elif cls == X_FWD:
            src, dst, dev = g_ref.at[2, 0, a, b], g_ref.at[3, 0, a, b], dev_x
        elif cls == S_OWN:
            src, dst, dev = own, g_ref.at[0, 1, a, b], dev_s
        elif cls == S_X:
            src, dst, dev = g_ref.at[1, 0, a, b], g_ref.at[1, 1, a, b], dev_s
        elif cls == S_Y:
            src, dst, dev = g_ref.at[2, 0, a, b], g_ref.at[2, 1, a, b], dev_s
        else:
            src, dst, dev = g_ref.at[3, 0, a, b], g_ref.at[3, 1, a, b], dev_s
        return pltpu.make_async_remote_copy(
            src_ref=src, dst_ref=dst, send_sem=send_sem.at[cls, n],
            recv_sem=recv_sem.at[cls, n], device_id=dev, device_id_type=MESH)

    def own_send(n):
        for cls in (X_DIR, Y_DIR, S_OWN):
            mk(cls, n).start()

    def forward(n):
        mk(X_DIR, n).wait_recv()
        mk(Y_FWD, n).start()
        mk(S_X, n).start()
        mk(Y_DIR, n).wait_recv()
        mk(X_FWD, n).start()
        mk(S_Y, n).start()

    def share_diag(n):
        mk(Y_FWD, n).wait_recv()
        mk(S_DA, n).start()
        mk(X_FWD, n).wait_recv()
        mk(S_DB, n).start()

    def sib_wait(n):
        for cls in (S_OWN, S_X, S_Y, S_DA, S_DB):
            mk(cls, n).wait_recv()

    def vloads(n):
        a, b = win(n)
        cps = []
        for k in range(4):
            for cc in range(2):
                src = v_ref.at[a, b] if (k == 0 and cc == 0) else g_ref.at[k, cc, a, b]
                cps.append(pltpu.make_async_copy(
                    src, vbuf.at[k, a, pl.ds(128 * cc, 128)], load_sem.at[2 * k + cc]))
        return cps

    t_local = pltpu.make_async_copy(t_ref, t_own, aux_sem.at[0])
    t_local.start()
    t_remote = pltpu.make_async_remote_copy(
        src_ref=t_ref, dst_ref=t_sib, send_sem=aux_sem.at[1], recv_sem=aux_sem.at[2],
        device_id=dev_s, device_id_type=MESH)
    t_remote.start()
    zl = [pltpu.make_async_copy(
        z_ref.at[pl.ds(pl.multiple_of(peer_row[k] * LOC_ROWS, LOC_ROWS), LOC_ROWS), :],
        stage.at[k], aux_sem.at[3 + k]) for k in range(4)]
    for cp in zl:
        cp.start()
    if comm:
        for n in OWN_AT[-1]:
            own_send(n)

    vbuf[...] = jnp.zeros_like(vbuf)
    dmat[...] = jnp.zeros_like(dmat)
    for cp in zl:
        cp.wait()

    @pl.loop(0, 32)
    def _(t):
        k, i4 = lax.rem(t, 4), t // 4
        xt[t] = stage[k, pl.ds(pl.multiple_of(i4 * TILE, TILE), TILE), :].T

    t_local.wait()
    t_remote.wait()
    if comm:
        for n in FWD_AT[-1]:
            forward(n)
        for n in DIAG_AT[-1]:
            share_diag(n)
        sib_wait(0)
    for cp in vloads(0):
        cp.start()

    def order(dim):
        pos = lax.broadcasted_iota(jnp.int32, (TILE, TILE), dim) // 64
        core = pos // 2
        return 2 * (pos - 2 * core) + core + c - 2 * core * c

    def block(n, hook):
        m = STEPS - 1 - n
        for i in range(2):
            dmat[64 * i:64 * i + 64, 64 * i:64 * i + 64] = t_own[2 * m + i]
            dmat[128 + 64 * i:192 + 64 * i, 128 + 64 * i:192 + 64 * i] = t_sib[2 * m + i]
        wt[...] = jnp.zeros_like(wt)
        gm[...] = jnp.zeros_like(gm)

        @pl.loop(m // 4, 8)
        def _(i4):
            rows = pl.ds(pl.multiple_of(i4 * TILE, TILE), TILE)
            vt, xl = [], []
            for k in range(4):
                v = split3(vbuf[k, rows, :])
                for i in range(3):
                    vs[i, 4 * i4 + k] = v[i]
                vt.append(v)
                xl.append(split3(xt[4 * i4 + k]))
            wt[...] += six(xl, vt, NN)
            high = [v[i] for v in vt for i in (0, 1)]
            high = jnp.concatenate(high, axis=0)
            gm[0] += dotb(high, high, TN)
            left = jnp.concatenate([v[0] for v in vt for i in (1, 2)], axis=0)
            right = jnp.concatenate([v[i] for v in vt for i in (1, 2)], axis=0)
            gm[1] += dotb(left, right, TN)

        hook()
        cross = gm[1]
        gram = gm[0] + cross + cross.T
        upper = jnp.where(order(0) < order(1), gram, 0.0)
        diag = dmat[...]
        nil = dot32(diag, upper)
        p0 = dot32(wt[...], diag, NT)
        p1 = dot32(p0, nil, NT)
        sq = dot32(nil, nil)
        p23 = dot32(jnp.concatenate([p0, p1], axis=0), sq, NT)
        y = split3((p0 - p1) + (p23[:TILE] - p23[TILE:]))
        for i in range(3):
            yt[i] = y[i]

        @pl.loop(jnp.where(n == STEPS - 1, 8, m // 4), 8)
        def _(i4):
            for k in range(4):
                t = 4 * i4 + k
                xt[t] -= six([(yt[0], yt[1], yt[2])], [(vs[0, t], vs[1, t], vs[2, t])], NT)

    def next_loads(n):
        if comm:
            sib_wait(n)
        for cp in vloads(n):
            cp.start()

    def each(n, body):
        for g in range(0, STEPS, 8):
            @pl.when(n // 8 == g // 8)
            def _(g=g):
                for k in range(g, g + 8):
                    pl.when(n == k)(functools.partial(body, k))

    def top(k):
        if comm:
            for n in OWN_AT[k]:
                own_send(n)
            for n in FWD_AT[k]:
                if n < STEPS - 1:
                    forward(n)
            for n in DIAG_AT[k]:
                if n < STEPS - 1:
                    share_diag(n)
        for cp in vloads(k):
            cp.wait()

    def middle(k):
        if comm and STEPS - 1 in FWD_AT[k]:
            forward(STEPS - 1)
        if k + 1 < STEPS - 2:
            next_loads(k + 1)

    @pl.loop(0, STEPS)
    def _(n):
        each(n, top)
        if compute:
            block(n, lambda: each(n, middle))
        else:
            each(n, middle)

        @pl.when(n == STEPS - 3)
        def _():
            next_loads(STEPS - 2)

        @pl.when(n == STEPS - 2)
        def _():
            if comm:
                share_diag(STEPS - 1)
            next_loads(STEPS - 1)

    finals = {}
    for k in (3, 1, 2, 0):
        @pl.loop(0, 8)
        def _(i4, k=k):
            t = 4 * i4 + k
            done = xt[t]
            if compute:
                done -= six([(yt[0], yt[1], yt[2])], [(vs[0, t], vs[1, t], vs[2, t])], NT)
            stage[k, pl.ds(pl.multiple_of(i4 * TILE, TILE), TILE), :] = done.T
        cols = out_ref.at[:, pl.ds(pl.multiple_of(r * TILE, TILE), TILE)]
        if k:
            finals[k] = pltpu.make_async_remote_copy(
                src_ref=stage.at[k], dst_ref=cols, send_sem=fin_send.at[k],
                recv_sem=fin_recv.at[k], device_id=(peer_row[k], c), device_id_type=MESH)
        else:
            finals[k] = pltpu.make_async_copy(stage.at[0], cols, fin_send.at[0])
        finals[k].start()
    if comm:
        for n in range(STEPS):
            for cls in range(9):
                mk(cls, n).wait_send()
    for k in range(4):
        finals[k].wait()


def solution(mesh, comm=True, compute=True):
    def local_body(v_loc, t_loc, z_loc):
        any_spec = pl.BlockSpec(memory_space=pl.ANY)
        out, _ = pl.pallas_call(
            functools.partial(kernel, comm=comm, compute=compute),
            out_shape=(jax.ShapeDtypeStruct((LOC_ROWS, 4 * TILE), F32),
                       jax.ShapeDtypeStruct((4, 2, LOC_ROWS, 4096), F32)),
            in_specs=[any_spec] * 3,
            out_specs=(any_spec, any_spec),
            scratch_shapes=[
                pltpu.VMEM((32, TILE, TILE), F32),
                pltpu.VMEM((4, LOC_ROWS, TILE), F32),
                pltpu.VMEM((3, 32, TILE, TILE), BF16),
                pltpu.VMEM((4, LOC_ROWS, TILE), F32),
                pltpu.VMEM((64, 64, 64), F32),
                pltpu.VMEM((64, 64, 64), F32),
                pltpu.VMEM((TILE, TILE), F32),
                pltpu.VMEM((TILE, TILE), F32),
                pltpu.VMEM((2, TILE, TILE), F32),
                pltpu.VMEM((3, TILE, TILE), BF16),
                pltpu.SemaphoreType.DMA((9, STEPS)),
                pltpu.SemaphoreType.DMA((9, STEPS)),
                pltpu.SemaphoreType.DMA((8,)),
                pltpu.SemaphoreType.DMA((7,)),
                pltpu.SemaphoreType.DMA((4,)),
                pltpu.SemaphoreType.DMA((4,)),
            ],
            compiler_params=pltpu.CompilerParams(
                collective_id=0, has_side_effects=True, vmem_limit_bytes=60 * 2**20),
            name="apply_panels",
        )(v_loc, t_loc, z_loc)
        return out

    return jax.shard_map(local_body, mesh=mesh,
                         in_specs=(P('row', 'col'), P('col', None, None), P(None, ('col', 'row'))),
                         out_specs=P('row', 'col'), check_vma=False)
```

```python
import functools

import jax
import jax.numpy as jnp
from jax import lax
from jax.experimental import pallas as pl
from jax.experimental.pallas import tpu as pltpu
from jax.sharding import PartitionSpec as P

MESH = pl.DeviceIdType.MESH
HIGHEST = lax.Precision.HIGHEST
F32, BF16 = jnp.float32, jnp.bfloat16

STEPS = 32
TILE = 256
LOC_ROWS = 2048


def ahead(n, early, late):
    return early if n < 14 else max(late, early - (n - 14))


def plan(early, late):
    at = {k: [] for k in range(-1, STEPS)}
    for n in range(STEPS):
        at[max(n - ahead(n, early, late), -1)].append(n)
    return at


OWN_AT = plan(6, 4)
FWD_AT = plan(4, 3)
DIAG_AT = plan(2, 1)

NN = (((1,), (0,)), ((), ()))
NT = (((1,), (1,)), ((), ()))
TN = (((0,), (0,)), ((), ()))


def dot32(a, b, dims=NN):
    return lax.dot_general(a, b, dims, precision=HIGHEST, preferred_element_type=F32)


def dotb(a, b, dims=NN):
    return lax.dot_general(a, b, dims, preferred_element_type=F32)


def split3(x):
    hi = x.astype(BF16)
    rest = x - hi.astype(F32)
    mid = rest.astype(BF16)
    low = (rest - mid.astype(F32)).astype(BF16)
    return hi, mid, low


def six(a, b, dims):
    (ldim,), (rdim,) = dims[0]
    lhs = [x[i] for x in a for i in (0, 0, 1, 1, 0, 2)]
    rhs = [x[i] for x in b for i in (0, 1, 0, 1, 2, 0)]
    return dotb(jnp.concatenate(lhs, axis=ldim), jnp.concatenate(rhs, axis=rdim), dims)


X_DIR, Y_DIR, Y_FWD, X_FWD, S_OWN, S_X, S_Y, S_DA, S_DB = range(9)


def kernel(v_ref, t_ref, z_ref, out_ref, g_ref,
           xt, vbuf, vs, stage, t_own, t_sib, dmat, wt, gm, yt,
           send_sem, recv_sem, load_sem, aux_sem, fin_send, fin_recv,
           *, comm=True, compute=True):
    r = lax.axis_index("row")
    c = lax.axis_index("col")
    rx = r + 1 - 2 * lax.rem(r, 2)
    ry = lax.rem(r + 2, 4)
    rd = 3 - r
    dev_x, dev_y, dev_d, dev_s = (rx, c), (ry, c), (rd, c), (r, 1 - c)
    peer_row = (r, rx, ry, rd)

    barrier = pltpu.get_barrier_semaphore()
    for dev in (dev_x, dev_y, dev_d, dev_s):
        pl.semaphore_signal(barrier, inc=1, device_id=dev, device_id_type=MESH)
    pl.semaphore_wait(barrier, 4)

    def win(n, part=None):
        m = STEPS - 1 - n
        lo, rows = 64 * m, 64 * (n + 1)
        if part == 0:
            rows = rows // 2
        elif part == 1:
            lo, rows = lo + rows // 2, rows // 2
        return pl.ds(lo, rows), pl.ds(128 * m, 128)

    def mk(cls, n):
        part = {Y_FWD: 0, S_DA: 0, X_FWD: 1, S_DB: 1}.get(cls)
        a, b = win(n, part)
        own = v_ref.at[a, b]
        if cls == X_DIR:
            src, dst, dev = own, g_ref.at[1, 0, a, b], dev_x
        elif cls == Y_DIR:
            src, dst, dev = own, g_ref.at[2, 0, a, b], dev_y
        elif cls == Y_FWD:
            src, dst, dev = g_ref.at[1, 0, a, b], g_ref.at[3, 0, a, b], dev_y
        elif cls == X_FWD:
            src, dst, dev = g_ref.at[2, 0, a, b], g_ref.at[3, 0, a, b], dev_x
        elif cls == S_OWN:
            src, dst, dev = own, g_ref.at[0, 1, a, b], dev_s
        elif cls == S_X:
            src, dst, dev = g_ref.at[1, 0, a, b], g_ref.at[1, 1, a, b], dev_s
        elif cls == S_Y:
            src, dst, dev = g_ref.at[2, 0, a, b], g_ref.at[2, 1, a, b], dev_s
        else:
            src, dst, dev = g_ref.at[3, 0, a, b], g_ref.at[3, 1, a, b], dev_s
        return pltpu.make_async_remote_copy(
            src_ref=src, dst_ref=dst, send_sem=send_sem.at[cls, n],
            recv_sem=recv_sem.at[cls, n], device_id=dev, device_id_type=MESH)

    def own_send(n):
        for cls in (X_DIR, Y_DIR, S_OWN):
            mk(cls, n).start()

    def forward(n):
        mk(X_DIR, n).wait_recv()
        mk(Y_FWD, n).start()
        mk(S_X, n).start()
        mk(Y_DIR, n).wait_recv()
        mk(X_FWD, n).start()
        mk(S_Y, n).start()

    def share_diag(n):
        mk(Y_FWD, n).wait_recv()
        mk(S_DA, n).start()
        mk(X_FWD, n).wait_recv()
        mk(S_DB, n).start()

    def sib_wait(n):
        for cls in (S_OWN, S_X, S_Y, S_DA, S_DB):
            mk(cls, n).wait_recv()

    def vloads(n):
        a, b = win(n)
        cps = []
        for k in range(4):
            for cc in range(2):
                src = v_ref.at[a, b] if (k == 0 and cc == 0) else g_ref.at[k, cc, a, b]
                cps.append(pltpu.make_async_copy(
                    src, vbuf.at[k, a, pl.ds(128 * cc, 128)], load_sem.at[2 * k + cc]))
        return cps

    t_local = pltpu.make_async_copy(t_ref, t_own, aux_sem.at[0])
    t_local.start()
    t_remote = pltpu.make_async_remote_copy(
        src_ref=t_ref, dst_ref=t_sib, send_sem=aux_sem.at[1], recv_sem=aux_sem.at[2],
        device_id=dev_s, device_id_type=MESH)
    t_remote.start()
    zl = [pltpu.make_async_copy(
        z_ref.at[pl.ds(pl.multiple_of(peer_row[k] * LOC_ROWS, LOC_ROWS), LOC_ROWS), :],
        stage.at[k], aux_sem.at[3 + k]) for k in range(4)]
    for cp in zl:
        cp.start()
    if comm:
        for n in OWN_AT[-1]:
            own_send(n)

    vbuf[...] = jnp.zeros_like(vbuf)
    dmat[...] = jnp.zeros_like(dmat)
    for cp in zl:
        cp.wait()

    @pl.loop(0, 32)
    def _(t):
        k, i4 = lax.rem(t, 4), t // 4
        xt[t] = stage[k, pl.ds(pl.multiple_of(i4 * TILE, TILE), TILE), :].T

    t_local.wait()
    t_remote.wait()
    if comm:
        for n in FWD_AT[-1]:
            forward(n)
        for n in DIAG_AT[-1]:
            share_diag(n)
        sib_wait(0)
    for cp in vloads(0):
        cp.start()

    def order(dim):
        pos = lax.broadcasted_iota(jnp.int32, (TILE, TILE), dim) // 64
        core = pos // 2
        return 2 * (pos - 2 * core) + core + c - 2 * core * c

    def block(n, hook):
        m = STEPS - 1 - n
        for i in range(2):
            dmat[64 * i:64 * i + 64, 64 * i:64 * i + 64] = t_own[2 * m + i]
            dmat[128 + 64 * i:192 + 64 * i, 128 + 64 * i:192 + 64 * i] = t_sib[2 * m + i]
        wt[...] = jnp.zeros_like(wt)
        gm[...] = jnp.zeros_like(gm)

        @pl.loop(m // 4, 8)
        def _(i4):
            rows = pl.ds(pl.multiple_of(i4 * TILE, TILE), TILE)
            vt, xl = [], []
            for k in range(4):
                v = split3(vbuf[k, rows, :])
                for i in range(3):
                    vs[i, 4 * i4 + k] = v[i]
                vt.append(v)
                xl.append(split3(xt[4 * i4 + k]))
            wt[...] += six(xl, vt, NN)
            high = [v[i] for v in vt for i in (0, 1)]
            high = jnp.concatenate(high, axis=0)
            gm[0] += dotb(high, high, TN)
            left = jnp.concatenate([v[0] for v in vt for i in (1, 2)], axis=0)
            right = jnp.concatenate([v[i] for v in vt for i in (1, 2)], axis=0)
            gm[1] += dotb(left, right, TN)

        hook()
        cross = gm[1]
        gram = gm[0] + cross + cross.T
        upper = jnp.where(order(0) < order(1), gram, 0.0)
        diag = dmat[...]
        nil = dot32(diag, upper)
        p0 = dot32(wt[...], diag, NT)
        p1 = dot32(p0, nil, NT)
        sq = dot32(nil, nil)
        p23 = dot32(jnp.concatenate([p0, p1], axis=0), sq, NT)
        y = split3((p0 - p1) + (p23[:TILE] - p23[TILE:]))
        for i in range(3):
            yt[i] = y[i]

        @pl.loop(jnp.where(n == STEPS - 1, 8, m // 4), 8)
        def _(i4):
            for k in range(4):
                t = 4 * i4 + k
                xt[t] -= six([(yt[0], yt[1], yt[2])], [(vs[0, t], vs[1, t], vs[2, t])], NT)

    def next_loads(n):
        if comm:
            sib_wait(n)
        for cp in vloads(n):
            cp.start()

    def each(n, body):
        for g in range(0, STEPS, 8):
            @pl.when(n // 8 == g // 8)
            def _(g=g):
                for k in range(g, g + 8):
                    pl.when(n == k)(functools.partial(body, k))

    def top(k):
        if comm:
            for n in OWN_AT[k]:
                own_send(n)
            for n in FWD_AT[k]:
                if n < STEPS - 1:
                    forward(n)
            for n in DIAG_AT[k]:
                if n < STEPS - 1:
                    share_diag(n)
        for cp in vloads(k):
            cp.wait()

    def middle(k):
        if comm and STEPS - 1 in FWD_AT[k]:
            forward(STEPS - 1)
        if k + 1 < STEPS - 2:
            next_loads(k + 1)

    @pl.loop(0, STEPS)
    def _(n):
        each(n, top)
        if compute:
            block(n, lambda: each(n, middle))
        else:
            each(n, middle)

        @pl.when(n == STEPS - 3)
        def _():
            next_loads(STEPS - 2)

        @pl.when(n == STEPS - 2)
        def _():
            if comm:
                share_diag(STEPS - 1)
            next_loads(STEPS - 1)

    finals = {}
    for k in (3, 1, 2, 0):
        @pl.loop(0, 8)
        def _(i4, k=k):
            t = 4 * i4 + k
            done = xt[t]
            if compute:
                done -= six([(yt[0], yt[1], yt[2])], [(vs[0, t], vs[1, t], vs[2, t])], NT)
            stage[k, pl.ds(pl.multiple_of(i4 * TILE, TILE), TILE), :] = done.T
        cols = out_ref.at[:, pl.ds(pl.multiple_of(r * TILE, TILE), TILE)]
        if k:
            finals[k] = pltpu.make_async_remote_copy(
                src_ref=stage.at[k], dst_ref=cols, send_sem=fin_send.at[k],
                recv_sem=fin_recv.at[k], device_id=(peer_row[k], c), device_id_type=MESH)
        else:
            finals[k] = pltpu.make_async_copy(stage.at[0], cols, fin_send.at[0])
        finals[k].start()
    if comm:
        for n in range(STEPS):
            for cls in range(9):
                mk(cls, n).wait_send()
    for k in range(4):
        finals[k].wait()


def solution(mesh, comm=True, compute=True):
    def local_body(v_loc, t_loc, z_loc):
        any_spec = pl.BlockSpec(memory_space=pl.ANY)
        out, _ = pl.pallas_call(
            functools.partial(kernel, comm=comm, compute=compute),
            out_shape=(jax.ShapeDtypeStruct((LOC_ROWS, 4 * TILE), F32),
                       jax.ShapeDtypeStruct((4, 2, LOC_ROWS, 4096), F32)),
            in_specs=[any_spec] * 3,
            out_specs=(any_spec, any_spec),
            scratch_shapes=[
                pltpu.VMEM((32, TILE, TILE), F32),
                pltpu.VMEM((4, LOC_ROWS, TILE), F32),
                pltpu.VMEM((3, 32, TILE, TILE), BF16),
                pltpu.VMEM((4, LOC_ROWS, TILE), F32),
                pltpu.VMEM((64, 64, 64), F32),
                pltpu.VMEM((64, 64, 64), F32),
                pltpu.VMEM((TILE, TILE), F32),
                pltpu.VMEM((TILE, TILE), F32),
                pltpu.VMEM((2, TILE, TILE), F32),
                pltpu.VMEM((3, TILE, TILE), BF16),
                pltpu.SemaphoreType.DMA((9, STEPS)),
                pltpu.SemaphoreType.DMA((9, STEPS)),
                pltpu.SemaphoreType.DMA((8,)),
                pltpu.SemaphoreType.DMA((7,)),
                pltpu.SemaphoreType.DMA((4,)),
                pltpu.SemaphoreType.DMA((4,)),
            ],
            compiler_params=pltpu.CompilerParams(
                collective_id=0, has_side_effects=True, vmem_limit_bytes=60 * 2**20),
            name="apply_panels",
        )(v_loc, t_loc, z_loc)
        return out

    return jax.shard_map(local_body, mesh=mesh,
                         in_specs=(P('row', 'col'), P('col', None, None), P(None, ('col', 'row'))),
                         out_specs=P('row', 'col'), check_vma=False)
```
